32 devices in a mesh: bx: 4 (over y, x), by: 8 (over z, core).
Axes of the slice: x: 2, y: 2, z: 4, core: 2. Of those that a mesh axis runs over, the one named last changes fastest.
Arguments:
- forcing: float32 [1216, 1024], P('by', 'bx'), may hold values from -20 to 20
- guess: float32 [1216, 1024], P('by', 'bx'), may hold values from -3 to 3
- shift: float32 [1216, 1024], P('by', 'bx'), may hold values from 0.05 to 2
- ocean_mask: int32 [1216, 1024], P('by', 'bx'), may hold values 0 or 1
Outputs:
- solution_field: float32 [1216, 1024], P('by', 'bx')
- residual: float32 [1216, 1024], P('by', 'bx')
- residual_norm: float32 [], replicated
The draws below stay inside these ranges and needn't reach their ends.
All inputs are finite; a program needn't handle non-finite values. No bound on the sum of `ocean_mask` on one device may be relied on, other than what follows from the above.
Results may differ from the reference program's by a relative error of at most 0.00002.
Values sent between devices are 32-bit elements; how exact they have to be, the bound alone decides.
A program may use at most 64 MiB of HBM per device.

```python
import math
import jax
import jax.numpy as jnp
from jax import lax

ITERS = 4
NX = 1024
NY = 1216


def draw_forcing(key, part):
    rows = jnp.arange(NY, dtype=jnp.float32)
    rising = 1.0 + 2.0 * rows / max(NY - 1, 1)
    rough = jnp.clip(jax.random.normal(key, (NY, NX), jnp.float32), -6.0, 6.0)
    values = rough * rising[:, None]
    return jnp.clip(values, -20.0, 20.0)


def touch_ends(entries, own_key, smallest, top_value):
    index_at = [jax.random.randint(jax.random.fold_in(own_key, axis), (), 0, length) for axis, length in enumerate(entries.shape)]
    widest = entries.shape.index(max(entries.shape))
    neighbour = index_at[:widest] + [(index_at[widest] + 1) % entries.shape[widest]] + index_at[widest + 1:]
    return entries.at[tuple(index_at)].set(smallest).at[tuple(neighbour)].set(top_value)


def levels(stream_key, dims, cuts, least, top_value):
    def one(axis_at, parts):
        draws = jax.random.uniform(jax.random.fold_in(jax.random.fold_in(stream_key, 6), axis_at), (parts,), jnp.float32, least / len(cuts), top_value / len(cuts))
        return jnp.repeat(jnp.exp(draws), dims[axis_at] // parts).reshape((-1,) + (1,) * (len(dims) - axis_at - 1))

    level = one(*cuts[0])
    for cut in cuts[1:]:
        level = level * one(*cut)
    return level


def scatter_about(key, shape, scale, reach, cuts=(), kind=jnp.bfloat16):
    entries = scale * jax.random.normal(key, shape, jnp.float32)
    if cuts:
        entries = entries * levels(key, shape, cuts, -0.22, 0.18)
    return jnp.clip(entries, -reach, reach).astype(kind)


def setup_inputs(seed: int = 0) -> dict:
    streams_of = jax.random.split(jax.random.key(seed), 5)
    return {
        "forcing": draw_forcing(jax.random.fold_in(streams_of[4], 71), 0),
        "guess": scatter_about(streams_of[1], (NY, NX), 0.5, 3.0, ((0, 8), (1, 4)), jnp.float32),
        "shift": jnp.clip(jnp.exp(math.log(2.0) - 3.6888794 * jax.random.uniform(streams_of[2], (NY, NX), jnp.float32) ** levels(streams_of[2], (NY, NX), ((0, 8), (1, 4)), -0.2, 0.2)), 0.05, 2.0),
        "ocean_mask": touch_ends((jax.random.randint(streams_of[3], (NY, NX), 0, 5) < 4).astype(jnp.int32), jax.random.fold_in(streams_of[3], 1), 0, 1),
    }


LOW_BOUND = 0.05
HIGH_BOUND = 14.5

def extend(values):
    zonal = jnp.concatenate([values[:, -1:], values, values[:, :1]], axis=1)
    top_row = zonal[-1, ::-1]
    bottom_row = jnp.zeros_like(top_row)
    return jnp.concatenate([bottom_row[None, :], zonal, top_row[None, :]], axis=0)

def nine_point(values, shift, mask_f):
    padded = extend(values)
    center = padded[1:-1, 1:-1]
    sides = padded[2:, 1:-1] + padded[:-2, 1:-1] + padded[1:-1, 2:] + padded[1:-1, :-2]
    corners = padded[2:, 2:] + padded[2:, :-2] + padded[:-2, 2:] + padded[:-2, :-2]
    return mask_f * ((6.0 + shift) * center - sides - 0.5 * corners)

def pair_add(first, second):
    total = first[0] + second[0]
    backed = total - first[0]
    error = first[0] - (total - backed) + (second[0] - backed)
    error = error + first[1] + second[1]
    upper = total + error
    lower = error - (upper - total)
    return (upper, lower)

def tree_total(uppers, lowers):
    while uppers.shape[0] > 1:
        if uppers.shape[0] % 2 == 1:
            uppers = jnp.concatenate([uppers, jnp.zeros((1,), uppers.dtype)])
            lowers = jnp.concatenate([lowers, jnp.zeros((1,), lowers.dtype)])
        uppers, lowers = pair_add((uppers[0::2], lowers[0::2]), (uppers[1::2], lowers[1::2]))
    return (uppers[0], lowers[0])

def reference(forcing, guess, shift, ocean_mask):
    mask_f = ocean_mask.astype(jnp.float32)
    theta = (HIGH_BOUND + LOW_BOUND) / 2.0
    delta = (HIGH_BOUND - LOW_BOUND) / 2.0
    sigma = theta / delta
    rho = 1.0 / sigma
    iterate = mask_f * guess
    resid = mask_f * forcing - nine_point(iterate, shift, mask_f)
    direction = resid / theta
    for sweep in range(ITERS):
        iterate = iterate + direction
        resid = resid - nine_point(direction, shift, mask_f)
        rho_next = 1.0 / (2.0 * sigma - rho)
        direction = rho_next * rho * direction + 2.0 * rho_next / delta * resid
        rho = rho_next
    row_sums = lax.optimization_barrier(jnp.sum(resid * resid, axis=1))
    upper, lower = tree_total(row_sums, jnp.zeros_like(row_sums))
    norm_value = jnp.sqrt((upper + lower) / (NX * NY))
    return (iterate, resid, norm_value)
```

```python
import functools

import jax
import jax.numpy as jnp
from jax import lax
from jax.experimental import pallas as pl
from jax.experimental.pallas import tpu as pltpu
from jax.sharding import PartitionSpec as P

ITERS = 4
LOW_BOUND = 0.05
HIGH_BOUND = 14.5

EDGE = 8
LANES = 128
FIELDS = 4
SW, SE, NW, NE = 0, 1, 2, 3
MESH_ID = pl.DeviceIdType.MESH


def pair_add(first, second):
    total = first[0] + second[0]
    backed = total - first[0]
    error = first[0] - (total - backed) + (second[0] - backed)
    error = error + first[1] + second[1]
    upper = total + error
    lower = error - (upper - total)
    return (upper, lower)


def pair_tree(pairs):
    while len(pairs) > 1:
        merged = [pair_add(pairs[i], pairs[i + 1]) for i in range(0, len(pairs) - 1, 2)]
        if len(pairs) % 2 == 1:
            merged.append(pairs[-1])
        pairs = merged
    return pairs[0]


def flip_tile(tile):
    lane = lax.broadcasted_iota(jnp.int32, tile.shape, 1)
    row = lax.broadcasted_iota(jnp.int32, tile.shape, 0)
    tile = jnp.take_along_axis(tile, tile.shape[1] - 1 - lane, axis=1)
    return jnp.take_along_axis(tile, tile.shape[0] - 1 - row, axis=0)


def turn(tile, shift):
    shift = shift % LANES
    return tile if shift == 0 else pltpu.roll(tile, shift, 1)


def kernel(
    sizes,
    f_in, g_in, s_in, m_in,
    x_out, r_out, norm_out,
    ext, ext_m, mask, flip_f, flip_m, pack, came, corner, flip_c, x_buf, r_buf, part, parts,
    load_sem, send_sem, recv_sem, part_send, part_recv, own_sem, out_sem,
):
    nbx, nby, rows, cols = sizes
    n = nbx * nby
    bx, by = lax.axis_index("bx"), lax.axis_index("by")
    me = bx * nby + by
    fold = by == nby - 1
    bottom = by == 0
    east, west = lax.rem(bx + 1, nbx), lax.rem(bx + nbx - 1, nbx)
    low, high = EDGE, EDGE + rows
    whole = high + EDGE
    tiles = rows // 8
    chunks = LANES // (FIELDS * EDGE)
    per_chunk = -(-tiles // chunks)
    top_chunk, top_slot = divmod(tiles - 1, per_chunk)
    top = pl.ds(8 * top_slot, 8)
    lane = lax.broadcasted_iota(jnp.int32, (8, LANES), 1)

    loads = [
        pltpu.make_async_copy(source, ext.at[k, pl.ds(low, rows), pl.ds(0, cols)], load_sem.at[k])
        for k, source in enumerate((f_in, g_in, s_in))
    ]
    loads.append(pltpu.make_async_copy(m_in, ext_m.at[pl.ds(low, rows), :], load_sem.at[3]))
    for copy in loads:
        copy.start()

    barrier = pltpu.get_barrier_semaphore()

    def greet(k, carry):
        other = lax.rem(me + k, n)
        pl.semaphore_signal(
            barrier, inc=1, device_id=(other // nby, lax.rem(other, nby)), device_id_type=MESH_ID
        )
        return carry

    lax.fori_loop(1, n, greet, 0)

    for copy in loads:
        copy.wait()

    packed = [[jnp.zeros((8, LANES), jnp.float32)] * per_chunk for _ in range(2)]
    for t in range(tiles):
        chunk, slot = divmod(t, per_chunk)
        here = pl.ds(low + 8 * t, 8)
        for f in range(FIELDS):
            group = chunk * FIELDS + f
            if f < 3:
                left, right = ext[f, here, :LANES], ext[f, here, cols - LANES : cols]
            else:
                left = ext_m[here, :LANES].astype(jnp.float32)
                right = ext_m[here, cols - LANES :].astype(jnp.float32)
            keep = lane // EDGE == group
            packed[0][slot] = jnp.where(keep, turn(left, EDGE * group), packed[0][slot])
            packed[1][slot] = jnp.where(keep, turn(right, EDGE * group + EDGE), packed[1][slot])
    for side in range(2):
        for slot in range(per_chunk):
            pack[side, 8 * slot : 8 * slot + 8, :] = packed[side][slot]

    @pl.when(fold)
    def _():
        last = pl.ds(high - 8, 8)
        count = cols // LANES
        for j in range(count):
            src = pl.ds((count - 1 - j) * LANES, LANES)
            dst = pl.ds(j * LANES, LANES)
            for f in range(3):
                flip_f[f, :, dst] = flip_tile(ext[f, last, src])
            flip_m[:, dst] = flip_tile(ext_m[last, src])
        for side in range(2):
            flip_c[side] = flip_tile(pack[side, top, :])

    @pl.when(bottom)
    def _():
        ext[:, 0:EDGE, 0:cols] = jnp.zeros((3, EDGE, cols), jnp.float32)
        ext_m[0:EDGE, :] = jnp.zeros((EDGE, cols), jnp.int32)
        corner[SW] = jnp.zeros((8, LANES), jnp.float32)
        corner[SE] = jnp.zeros((8, LANES), jnp.float32)

    pl.semaphore_wait(barrier, n - 1)

    south_rows, north_rows = pl.ds(0, EDGE), pl.ds(high, EDGE)
    body = pl.ds(0, cols)

    def send(src, dst, slot, order, target):
        return pltpu.make_async_remote_copy(
            src_ref=src, dst_ref=dst, send_sem=send_sem.at[order], recv_sem=recv_sem.at[slot],
            device_id=target, device_id_type=MESH_ID,
        )

    to_west = send(pack.at[0], came.at[0], 8, 0, (west, by))
    to_east = send(pack.at[1], came.at[1], 9, 1, (east, by))

    south = lax.max(by - 1, 0)
    first_rows = pl.ds(low, EDGE)
    last_rows = pl.ds(high - EDGE, EDGE)
    to_south = [
        send(pack.at[0, pl.ds(0, 8), :], corner.at[NE], NE, 4, (west, south)),
        send(pack.at[1, pl.ds(0, 8), :], corner.at[NW], NW, 5, (east, south)),
        send(ext.at[:, first_rows, body], ext.at[:, north_rows, body], 6, 2, (bx, south)),
        send(ext_m.at[first_rows, :], ext_m.at[north_rows, :], 7, 3, (bx, south)),
    ]
    north = lax.min(by + 1, nby - 1)
    to_north = [
        send(pack.at[0, top, :], corner.at[SE], SE, 8, (west, north)),
        send(pack.at[1, top, :], corner.at[SW], SW, 9, (east, north)),
        send(ext.at[:, last_rows, body], ext.at[:, south_rows, body], 4, 6, (bx, north)),
        send(ext_m.at[last_rows, :], ext_m.at[south_rows, :], 5, 7, (bx, north)),
    ]
    partner = nbx - 1 - bx
    partner_east = lax.rem(partner + 1, nbx)
    partner_west = lax.rem(partner + nbx - 1, nbx)
    over_fold = [
        send(flip_f, ext.at[:, north_rows, body], 6, 6, (partner, by)),
        send(flip_m, ext_m.at[north_rows, :], 7, 7, (partner, by)),
    ]
    fold_corners = [
        (send(flip_c.at[0], corner.at[NW], NW, 8, (partner_east, by)),
         pltpu.make_async_copy(flip_c.at[0], corner.at[NW], recv_sem.at[NW]), partner_east),
        (send(flip_c.at[1], corner.at[NE], NE, 9, (partner_west, by)),
         pltpu.make_async_copy(flip_c.at[1], corner.at[NE], recv_sem.at[NE]), partner_west),
    ]

    @pl.when(jnp.logical_not(bottom))
    def _():
        for copy in to_south:
            copy.start()

    @pl.when(jnp.logical_not(fold))
    def _():
        for copy in to_north:
            copy.start()

    @pl.when(fold)
    def _():
        for remote, local, target in fold_corners:
            pl.when(target != bx)(remote.start)
            pl.when(target == bx)(local.start)
        for copy in over_fold:
            copy.start()

    to_west.start()
    to_east.start()

    to_west.wait_recv()
    to_east.wait_recv()

    for t in range(tiles):
        chunk, slot = divmod(t, per_chunk)
        here = pl.ds(low + 8 * t, 8)
        from_east = came[0, 8 * slot : 8 * slot + 8, :]
        from_west = came[1, 8 * slot : 8 * slot + 8, :]
        for f in range(FIELDS):
            group = chunk * FIELDS + f
            value = jnp.where(
                lane < EDGE,
                turn(from_east, -EDGE * group),
                jnp.where(lane >= LANES - EDGE, turn(from_west, -EDGE - EDGE * group), 0.0),
            )
            if f < 3:
                ext[f, here, cols:] = value
            else:
                mask[here, cols:] = value

    @pl.when(jnp.logical_not(bottom))
    def _():
        to_north[0].wait_recv()
        to_north[1].wait_recv()
        to_north[2].wait_recv()
        to_north[3].wait_recv()

    for copy in to_south:
        copy.wait_recv()

    corners = [corner[k] for k in range(4)]
    for f in range(FIELDS):
        group = top_chunk * FIELDS + f
        flipped = LANES // EDGE - 1 - group
        south_tile = jnp.where(
            lane < EDGE,
            turn(corners[SE], -EDGE * group),
            jnp.where(lane >= LANES - EDGE, turn(corners[SW], -EDGE - EDGE * group), 0.0),
        )
        north_east = jnp.where(
            fold, turn(corners[NE], -EDGE * flipped), turn(corners[NE], -EDGE * f)
        )
        north_west = jnp.where(
            fold, turn(corners[NW], -EDGE - EDGE * flipped), turn(corners[NW], -EDGE - EDGE * f)
        )
        north_tile = jnp.where(
            lane < EDGE, north_east, jnp.where(lane >= LANES - EDGE, north_west, 0.0)
        )
        if f < 3:
            ext[f, south_rows, cols:] = south_tile
            ext[f, north_rows, cols:] = north_tile
        else:
            mask[south_rows, cols:] = south_tile
            mask[north_rows, cols:] = north_tile
    mask[:, :cols] = ext_m[...].astype(jnp.float32)

    width = cols + LANES
    theta = (HIGH_BOUND + LOW_BOUND) / 2.0
    delta = (HIGH_BOUND - LOW_BOUND) / 2.0
    sigma = theta / delta
    rho = 1.0 / sigma

    wet = mask[...]
    diagonal = wet * (6.0 + ext[2])

    def apply(values):
        across = pltpu.roll(values, 1, 1) + pltpu.roll(values, width - 1, 1)
        column = values + 0.5 * across
        around = across + pltpu.roll(column, 1, 0) + pltpu.roll(column, whole - 1, 0)
        return diagonal * values - wet * around

    iterate = wet * ext[1]
    resid = wet * ext[0] - apply(iterate)
    direction = resid * (1.0 / theta)
    for sweep in range(ITERS):
        iterate = iterate + direction
        resid = resid - apply(direction)
        rho_next = 1.0 / (2.0 * sigma - rho)
        if sweep < ITERS - 1:
            direction = (rho_next * rho) * direction + (2.0 * rho_next / delta) * resid
        rho = rho_next

    final = resid[low:high, :cols]
    x_buf[...] = iterate[low:high, :cols]
    r_buf[...] = final
    out_x = pltpu.make_async_copy(x_buf, x_out, out_sem.at[0])
    out_r = pltpu.make_async_copy(r_buf, r_out, out_sem.at[1])
    out_x.start()
    out_r.start()

    square = final * final
    row_sums = jnp.sum(square, axis=1, keepdims=True)
    zero = jnp.zeros((8, 1), jnp.float32)
    pair = pair_tree([(row_sums[8 * t : 8 * t + 8], zero) for t in range(tiles)])
    pair = [jnp.broadcast_to(word, (8, LANES)) for word in pair]
    for step in (4, 2, 1):
        pair = pair_add(pair, [pltpu.roll(word, step, 0) for word in pair])
    part[...] = jnp.where(lane < LANES // 2, pair[0], pair[1])[0:1]

    def share(k):
        other = lax.rem(me + k, n)
        return pltpu.make_async_remote_copy(
            src_ref=part, dst_ref=parts.at[me], send_sem=part_send.at[k], recv_sem=part_recv.at[me],
            device_id=(other // nby, lax.rem(other, nby)), device_id_type=MESH_ID,
        )

    def begin(k, carry):
        share(k).start()
        return carry

    lax.fori_loop(1, n, begin, 0)
    parts[me] = part[...]

    to_west.wait_send()
    to_east.wait_send()

    @pl.when(jnp.logical_not(bottom))
    def _():
        for copy in to_south:
            copy.wait_send()

    @pl.when(jnp.logical_not(fold))
    def _():
        for copy in to_north:
            copy.wait_send()

    @pl.when(fold)
    def _():
        for remote, local, target in fold_corners:
            pl.when(target != bx)(remote.wait_send)
        for copy in over_fold:
            copy.wait_send()

    def finish(k, carry):
        share(k).wait_send()
        source = lax.rem(me + k, n)
        pltpu.make_async_copy(part, parts.at[source], part_recv.at[source]).wait()
        return carry

    lax.fori_loop(1, n, finish, 0)

    def words(i):
        row = parts[i]
        return row, pltpu.roll(row, LANES // 2, 1)

    upper, lower = pair_tree([words(i) for i in range(n)])
    norm_out[...] = jnp.sqrt((upper + lower) / (rows * cols * n))[:, 0:1]
    out_x.wait()
    out_r.wait()


def per_device(sizes, forcing, guess, shift, ocean_mask):
    nbx, nby, rows, cols = sizes
    n = nbx * nby
    whole, width = rows + 2 * EDGE, cols + LANES
    chunks = LANES // (FIELDS * EDGE)
    pack_rows = 8 * -(-(rows // 8) // chunks)
    f32 = jnp.float32
    hbm = pl.BlockSpec(memory_space=pl.ANY)
    x, r, norm = pl.pallas_call(
        functools.partial(kernel, sizes),
        out_shape=(
            jax.ShapeDtypeStruct((rows, cols), f32),
            jax.ShapeDtypeStruct((rows, cols), f32),
            jax.ShapeDtypeStruct((1, 1), f32),
        ),
        in_specs=[hbm] * 4,
        out_specs=(hbm, hbm, pl.BlockSpec(memory_space=pltpu.VMEM)),
        scratch_shapes=[
            pltpu.VMEM((3, whole, width), f32),
            pltpu.VMEM((whole, cols), jnp.int32),
            pltpu.VMEM((whole, width), f32),
            pltpu.VMEM((3, EDGE, cols), f32),
            pltpu.VMEM((EDGE, cols), jnp.int32),
            pltpu.VMEM((2, pack_rows, LANES), f32),
            pltpu.VMEM((2, pack_rows, LANES), f32),
            pltpu.VMEM((4, 8, LANES), f32),
            pltpu.VMEM((2, 8, LANES), f32),
            pltpu.VMEM((rows, cols), f32),
            pltpu.VMEM((rows, cols), f32),
            pltpu.VMEM((1, LANES), f32),
            pltpu.VMEM((n, 1, LANES), f32),
            pltpu.SemaphoreType.DMA((4,)),
            pltpu.SemaphoreType.DMA((10,)),
            pltpu.SemaphoreType.DMA((10,)),
            pltpu.SemaphoreType.DMA((n,)),
            pltpu.SemaphoreType.DMA((n,)),
            pltpu.SemaphoreType.DMA((1,)),
            pltpu.SemaphoreType.DMA((2,)),
        ],
        compiler_params=pltpu.CompilerParams(collective_id=0, has_side_effects=True),
        name="chebyshev",
    )(forcing, guess, shift, ocean_mask)
    return x, r, norm.reshape(())


def solution(mesh):
    spec = P("by", "bx")
    nbx, nby = mesh.shape["bx"], mesh.shape["by"]

    def run(forcing, guess, shift, ocean_mask):
        sizes = (nbx, nby, forcing.shape[0] // nby, forcing.shape[1] // nbx)
        return jax.shard_map(
            functools.partial(per_device, sizes),
            mesh=mesh,
            in_specs=(spec,) * 4,
            out_specs=(spec, spec, P()),
            check_vma=False,
        )(forcing, guess, shift, ocean_mask)

    return run
```

```python
import functools

import jax
import jax.numpy as jnp
from jax import lax
from jax.experimental import pallas as pl
from jax.experimental.pallas import tpu as pltpu
from jax.sharding import PartitionSpec as P

ITERS = 4
LOW_BOUND = 0.05
HIGH_BOUND = 14.5

EDGE = 8
LANES = 128
FIELDS = 4
SW, SE, NW, NE = 0, 1, 2, 3
MESH_ID = pl.DeviceIdType.MESH


def pair_add(first, second):
    total = first[0] + second[0]
    backed = total - first[0]
    error = first[0] - (total - backed) + (second[0] - backed)
    error = error + first[1] + second[1]
    upper = total + error
    lower = error - (upper - total)
    return (upper, lower)


def pair_tree(pairs):
    while len(pairs) > 1:
        merged = [pair_add(pairs[i], pairs[i + 1]) for i in range(0, len(pairs) - 1, 2)]
        if len(pairs) % 2 == 1:
            merged.append(pairs[-1])
        pairs = merged
    return pairs[0]


def flip_tile(tile):
    lane = lax.broadcasted_iota(jnp.int32, tile.shape, 1)
    row = lax.broadcasted_iota(jnp.int32, tile.shape, 0)
    tile = jnp.take_along_axis(tile, tile.shape[1] - 1 - lane, axis=1)
    return jnp.take_along_axis(tile, tile.shape[0] - 1 - row, axis=0)


def turn(tile, shift):
    shift = shift % LANES
    return tile if shift == 0 else pltpu.roll(tile, shift, 1)


def kernel(
    sizes,
    f_in, g_in, s_in, m_in,
    x_buf, r_buf, norm_out,
    ext, ext_m, mask, flip_f, flip_m, pack, came, corner, flip_c, part, parts,
    load_sem, send_sem, recv_sem, part_send, part_recv,
):
    nbx, nby, rows, cols = sizes
    n = nbx * nby
    bx, by = lax.axis_index("bx"), lax.axis_index("by")
    me = bx * nby + by
    fold = by == nby - 1
    bottom = by == 0
    east, west = lax.rem(bx + 1, nbx), lax.rem(bx + nbx - 1, nbx)
    low, high = EDGE, EDGE + rows
    whole = high + EDGE
    tiles = rows // 8
    chunks = LANES // (FIELDS * EDGE)
    per_chunk = -(-tiles // chunks)
    top_chunk, top_slot = divmod(tiles - 1, per_chunk)
    top = pl.ds(8 * top_slot, 8)
    lane = lax.broadcasted_iota(jnp.int32, (8, LANES), 1)

    loads = [
        pltpu.make_async_copy(source, ext.at[k, pl.ds(low, rows), pl.ds(0, cols)], load_sem.at[k])
        for k, source in enumerate((f_in, g_in, s_in))
    ]
    loads.append(pltpu.make_async_copy(m_in, ext_m.at[pl.ds(low, rows), :], load_sem.at[3]))
    for copy in loads:
        copy.start()

    barrier = pltpu.get_barrier_semaphore()

    def greet(k, carry):
        other = lax.rem(me + k, n)
        pl.semaphore_signal(
            barrier, inc=1, device_id=(other // nby, lax.rem(other, nby)), device_id_type=MESH_ID
        )
        return carry

    lax.fori_loop(1, n, greet, 0)

    for copy in loads:
        copy.wait()

    packed = [[jnp.zeros((8, LANES), jnp.float32)] * per_chunk for _ in range(2)]
    for t in range(tiles):
        chunk, slot = divmod(t, per_chunk)
        here = pl.ds(low + 8 * t, 8)
        for f in range(FIELDS):
            group = chunk * FIELDS + f
            if f < 3:
                left, right = ext[f, here, :LANES], ext[f, here, cols - LANES : cols]
            else:
                left = ext_m[here, :LANES].astype(jnp.float32)
                right = ext_m[here, cols - LANES :].astype(jnp.float32)
            keep = lane // EDGE == group
            packed[0][slot] = jnp.where(keep, turn(left, EDGE * group), packed[0][slot])
            packed[1][slot] = jnp.where(keep, turn(right, EDGE * group + EDGE), packed[1][slot])
    for side in range(2):
        for slot in range(per_chunk):
            pack[side, 8 * slot : 8 * slot + 8, :] = packed[side][slot]

    @pl.when(fold)
    def _():
        last = pl.ds(high - 8, 8)
        count = cols // LANES
        for j in range(count):
            src = pl.ds((count - 1 - j) * LANES, LANES)
            dst = pl.ds(j * LANES, LANES)
            for f in range(3):
                flip_f[f, :, dst] = flip_tile(ext[f, last, src])
            flip_m[:, dst] = flip_tile(ext_m[last, src])
        for side in range(2):
            flip_c[side] = flip_tile(pack[side, top, :])

    @pl.when(bottom)
    def _():
        ext[:, 0:EDGE, 0:cols] = jnp.zeros((3, EDGE, cols), jnp.float32)
        ext_m[0:EDGE, :] = jnp.zeros((EDGE, cols), jnp.int32)
        corner[SW] = jnp.zeros((8, LANES), jnp.float32)
        corner[SE] = jnp.zeros((8, LANES), jnp.float32)

    pl.semaphore_wait(barrier, n - 1)

    south_rows, north_rows = pl.ds(0, EDGE), pl.ds(high, EDGE)
    body = pl.ds(0, cols)

    def send(src, dst, slot, order, target):
        return pltpu.make_async_remote_copy(
            src_ref=src, dst_ref=dst, send_sem=send_sem.at[order], recv_sem=recv_sem.at[slot],
            device_id=target, device_id_type=MESH_ID,
        )

    to_west = send(pack.at[0], came.at[0], 8, 0, (west, by))
    to_east = send(pack.at[1], came.at[1], 9, 1, (east, by))

    south = lax.max(by - 1, 0)
    first_rows = pl.ds(low, EDGE)
    last_rows = pl.ds(high - EDGE, EDGE)
    to_south = [
        send(pack.at[0, pl.ds(0, 8), :], corner.at[NE], NE, 4, (west, south)),
        send(pack.at[1, pl.ds(0, 8), :], corner.at[NW], NW, 5, (east, south)),
        send(ext.at[:, first_rows, body], ext.at[:, north_rows, body], 6, 2, (bx, south)),
        send(ext_m.at[first_rows, :], ext_m.at[north_rows, :], 7, 3, (bx, south)),
    ]
    north = lax.min(by + 1, nby - 1)
    to_north = [
        send(pack.at[0, top, :], corner.at[SE], SE, 8, (west, north)),
        send(pack.at[1, top, :], corner.at[SW], SW, 9, (east, north)),
        send(ext.at[:, last_rows, body], ext.at[:, south_rows, body], 4, 6, (bx, north)),
        send(ext_m.at[last_rows, :], ext_m.at[south_rows, :], 5, 7, (bx, north)),
    ]
    partner = nbx - 1 - bx
    partner_east = lax.rem(partner + 1, nbx)
    partner_west = lax.rem(partner + nbx - 1, nbx)
    over_fold = [
        send(flip_f, ext.at[:, north_rows, body], 6, 6, (partner, by)),
        send(flip_m, ext_m.at[north_rows, :], 7, 7, (partner, by)),
    ]
    fold_corners = [
        (send(flip_c.at[0], corner.at[NW], NW, 8, (partner_east, by)),
         pltpu.make_async_copy(flip_c.at[0], corner.at[NW], recv_sem.at[NW]), partner_east),
        (send(flip_c.at[1], corner.at[NE], NE, 9, (partner_west, by)),
         pltpu.make_async_copy(flip_c.at[1], corner.at[NE], recv_sem.at[NE]), partner_west),
    ]

    @pl.when(jnp.logical_not(bottom))
    def _():
        for copy in to_south[:2]:
            copy.start()

    @pl.when(jnp.logical_not(fold))
    def _():
        for copy in to_north[:2]:
            copy.start()

    to_west.start()
    to_east.start()

    @pl.when(jnp.logical_not(bottom))
    def _():
        for copy in to_south[2:]:
            copy.start()

    @pl.when(jnp.logical_not(fold))
    def _():
        for copy in to_north[2:]:
            copy.start()

    @pl.when(fold)
    def _():
        for copy in over_fold:
            copy.start()
        for remote, local, target in fold_corners:
            pl.when(target != bx)(remote.start)
            pl.when(target == bx)(local.start)

    to_west.wait_recv()
    to_east.wait_recv()

    for t in range(tiles):
        chunk, slot = divmod(t, per_chunk)
        here = pl.ds(low + 8 * t, 8)
        from_east = came[0, 8 * slot : 8 * slot + 8, :]
        from_west = came[1, 8 * slot : 8 * slot + 8, :]
        for f in range(FIELDS):
            group = chunk * FIELDS + f
            value = jnp.where(
                lane < EDGE,
                turn(from_east, -EDGE * group),
                jnp.where(lane >= LANES - EDGE, turn(from_west, -EDGE - EDGE * group), 0.0),
            )
            if f < 3:
                ext[f, here, cols:] = value
            else:
                mask[here, cols:] = value

    @pl.when(jnp.logical_not(bottom))
    def _():
        to_north[0].wait_recv()
        to_north[1].wait_recv()
        to_north[2].wait_recv()
        to_north[3].wait_recv()

    for copy in to_south:
        copy.wait_recv()

    corners = [corner[k] for k in range(4)]
    for f in range(FIELDS):
        group = top_chunk * FIELDS + f
        flipped = LANES // EDGE - 1 - group
        south_tile = jnp.where(
            lane < EDGE,
            turn(corners[SE], -EDGE * group),
            jnp.where(lane >= LANES - EDGE, turn(corners[SW], -EDGE - EDGE * group), 0.0),
        )
        north_east = jnp.where(
            fold, turn(corners[NE], -EDGE * flipped), turn(corners[NE], -EDGE * f)
        )
        north_west = jnp.where(
            fold, turn(corners[NW], -EDGE - EDGE * flipped), turn(corners[NW], -EDGE - EDGE * f)
        )
        north_tile = jnp.where(
            lane < EDGE, north_east, jnp.where(lane >= LANES - EDGE, north_west, 0.0)
        )
        if f < 3:
            ext[f, south_rows, cols:] = south_tile
            ext[f, north_rows, cols:] = north_tile
        else:
            mask[south_rows, cols:] = south_tile
            mask[north_rows, cols:] = north_tile
    mask[:, :cols] = ext_m[...].astype(jnp.float32)

    width = cols + LANES
    theta = (HIGH_BOUND + LOW_BOUND) / 2.0
    delta = (HIGH_BOUND - LOW_BOUND) / 2.0
    sigma = theta / delta
    rho = 1.0 / sigma

    wet = mask[...]
    diagonal = wet * (6.0 + ext[2])

    def apply(values):
        across = pltpu.roll(values, 1, 1) + pltpu.roll(values, width - 1, 1)
        column = values + 0.5 * across
        around = across + pltpu.roll(column, 1, 0) + pltpu.roll(column, whole - 1, 0)
        return diagonal * values - wet * around

    iterate = wet * ext[1]
    resid = wet * ext[0] - apply(iterate)
    direction = resid * (1.0 / theta)
    for sweep in range(ITERS):
        iterate = iterate + direction
        resid = resid - apply(direction)
        rho_next = 1.0 / (2.0 * sigma - rho)
        if sweep < ITERS - 1:
            direction = (rho_next * rho) * direction + (2.0 * rho_next / delta) * resid
        rho = rho_next

    final = resid[low:high, :cols]
    x_buf[...] = iterate[low:high, :cols]
    r_buf[...] = final

    square = final * final
    row_sums = jnp.sum(square, axis=1, keepdims=True)
    zero = jnp.zeros((8, 1), jnp.float32)
    pair = pair_tree([(row_sums[8 * t : 8 * t + 8], zero) for t in range(tiles)])
    pair = [jnp.broadcast_to(word, (8, LANES)) for word in pair]
    for step in (4, 2, 1):
        pair = pair_add(pair, [pltpu.roll(word, step, 0) for word in pair])
    part[...] = jnp.where(lane < LANES // 2, pair[0], pair[1])[0:1]

    def share(k):
        other = lax.rem(me + k, n)
        return pltpu.make_async_remote_copy(
            src_ref=part, dst_ref=parts.at[me], send_sem=part_send.at[0], recv_sem=part_recv.at[0],
            device_id=(other // nby, lax.rem(other, nby)), device_id_type=MESH_ID,
        )

    def begin(k, carry):
        share(k).start()
        return carry

    lax.fori_loop(1, n, begin, 0)
    parts[me] = part[...]

    to_west.wait_send()
    to_east.wait_send()

    @pl.when(jnp.logical_not(bottom))
    def _():
        for copy in to_south:
            copy.wait_send()

    @pl.when(jnp.logical_not(fold))
    def _():
        for copy in to_north:
            copy.wait_send()

    @pl.when(fold)
    def _():
        for remote, local, target in fold_corners:
            pl.when(target != bx)(remote.wait_send)
        for copy in over_fold:
            copy.wait_send()

    others = parts.at[pl.ds(0, n - 1)]
    pltpu.make_async_copy(others, others, part_send.at[0]).wait()
    pltpu.make_async_copy(others, others, part_recv.at[0]).wait()

    def words(i):
        row = parts[i]
        return row, pltpu.roll(row, LANES // 2, 1)

    upper, lower = pair_tree([words(i) for i in range(n)])
    norm_out[...] = jnp.sqrt((upper + lower) / (rows * cols * n))[:, 0:1]


def write_out(x_in, r_in, x_out, r_out, sem):
    copies = [
        pltpu.make_async_copy(x_in, x_out, sem.at[0]),
        pltpu.make_async_copy(r_in, r_out, sem.at[1]),
    ]
    for copy in copies:
        copy.start()
    for copy in copies:
        copy.wait()


def per_device(sizes, forcing, guess, shift, ocean_mask):
    nbx, nby, rows, cols = sizes
    n = nbx * nby
    whole, width = rows + 2 * EDGE, cols + LANES
    chunks = LANES // (FIELDS * EDGE)
    pack_rows = 8 * -(-(rows // 8) // chunks)
    f32 = jnp.float32
    hbm = pl.BlockSpec(memory_space=pl.ANY)
    vmem = pl.BlockSpec(memory_space=pltpu.VMEM)
    x, r, norm = pl.pallas_call(
        functools.partial(kernel, sizes),
        out_shape=(
            pltpu.VMEM((rows, cols), f32),
            pltpu.VMEM((rows, cols), f32),
            jax.ShapeDtypeStruct((1, 1), f32),
        ),
        in_specs=[hbm] * 4,
        out_specs=(vmem, vmem, vmem),
        scratch_shapes=[
            pltpu.VMEM((3, whole, width), f32),
            pltpu.VMEM((whole, cols), jnp.int32),
            pltpu.VMEM((whole, width), f32),
            pltpu.VMEM((3, EDGE, cols), f32),
            pltpu.VMEM((EDGE, cols), jnp.int32),
            pltpu.VMEM((2, pack_rows, LANES), f32),
            pltpu.VMEM((2, pack_rows, LANES), f32),
            pltpu.VMEM((4, 8, LANES), f32),
            pltpu.VMEM((2, 8, LANES), f32),
            pltpu.VMEM((1, LANES), f32),
            pltpu.VMEM((n, 1, LANES), f32),
            pltpu.SemaphoreType.DMA((4,)),
            pltpu.SemaphoreType.DMA((10,)),
            pltpu.SemaphoreType.DMA((10,)),
            pltpu.SemaphoreType.DMA((1,)),
            pltpu.SemaphoreType.DMA((1,)),
        ],
        compiler_params=pltpu.CompilerParams(collective_id=0, has_side_effects=True),
        name="chebyshev",
    )(forcing, guess, shift, ocean_mask)
    x = pltpu.with_memory_space_constraint(x, pltpu.VMEM)
    r = pltpu.with_memory_space_constraint(r, pltpu.VMEM)
    field = jax.ShapeDtypeStruct((rows, cols), f32)
    x, r = pl.pallas_call(
        write_out,
        out_shape=(field, field),
        in_specs=[hbm] * 2,
        out_specs=(hbm, hbm),
        scratch_shapes=[pltpu.SemaphoreType.DMA((2,))],
        name="write_out",
    )(x, r)
    return x, r, norm.reshape(())


def solution(mesh):
    spec = P("by", "bx")
    nbx, nby = mesh.shape["bx"], mesh.shape["by"]

    def run(forcing, guess, shift, ocean_mask):
        sizes = (nbx, nby, forcing.shape[0] // nby, forcing.shape[1] // nbx)
        return jax.shard_map(
            functools.partial(per_device, sizes),
            mesh=mesh,
            in_specs=(spec,) * 4,
            out_specs=(spec, spec, P()),
            check_vma=False,
        )(forcing, guess, shift, ocean_mask)

    return run
```

```python
import functools

import jax
import jax.numpy as jnp
from jax import lax
from jax.experimental import pallas as pl
from jax.experimental.pallas import tpu as pltpu
from jax.sharding import PartitionSpec as P

ITERS = 4
LOW_BOUND = 0.05
HIGH_BOUND = 14.5

EDGE = 8
LANES = 128
FIELDS = 4
SW, SE, NW, NE = 0, 1, 2, 3
MESH_ID = pl.DeviceIdType.MESH


def pair_add(first, second):
    total = first[0] + second[0]
    backed = total - first[0]
    error = first[0] - (total - backed) + (second[0] - backed)
    error = error + first[1] + second[1]
    upper = total + error
    lower = error - (upper - total)
    return (upper, lower)


def pair_tree(pairs):
    while len(pairs) > 1:
        merged = [pair_add(pairs[i], pairs[i + 1]) for i in range(0, len(pairs) - 1, 2)]
        if len(pairs) % 2 == 1:
            merged.append(pairs[-1])
        pairs = merged
    return pairs[0]


def flip_tile(tile):
    lane = lax.broadcasted_iota(jnp.int32, tile.shape, 1)
    row = lax.broadcasted_iota(jnp.int32, tile.shape, 0)
    tile = jnp.take_along_axis(tile, tile.shape[1] - 1 - lane, axis=1)
    return jnp.take_along_axis(tile, tile.shape[0] - 1 - row, axis=0)


def turn(tile, shift):
    shift = shift % LANES
    return tile if shift == 0 else pltpu.roll(tile, shift, 1)


def other_devices(bx, by, nbx, nby):
    order = sorted(range(nby), key=lambda k: -min(k, nby - k))
    return [
        (lax.rem(bx + i, nbx), lax.rem(by + k, nby))
        for k in order
        for i in reversed(range(nbx))
        if i or k
    ]


def kernel(
    sizes,
    f_in, g_in, s_in, m_in,
    x_buf, r_buf, norm_out,
    ext, ext_m, mask, flip_f, flip_m, pack, came, corner, flip_c, part, parts,
    load_sem, send_sem, recv_sem, part_send, part_recv,
):
    nbx, nby, rows, cols = sizes
    n = nbx * nby
    bx, by = lax.axis_index("bx"), lax.axis_index("by")
    me = bx * nby + by
    fold = by == nby - 1
    bottom = by == 0
    east, west = lax.rem(bx + 1, nbx), lax.rem(bx + nbx - 1, nbx)
    low, high = EDGE, EDGE + rows
    whole = high + EDGE
    tiles = rows // 8
    chunks = LANES // (FIELDS * EDGE)
    per_chunk = -(-tiles // chunks)
    top_chunk, top_slot = divmod(tiles - 1, per_chunk)
    top = pl.ds(8 * top_slot, 8)
    lane = lax.broadcasted_iota(jnp.int32, (8, LANES), 1)

    barrier = pltpu.get_barrier_semaphore()
    others = other_devices(bx, by, nbx, nby)
    for other in others:
        pl.semaphore_signal(barrier, inc=1, device_id=other, device_id_type=MESH_ID)

    loads = [
        pltpu.make_async_copy(source, ext.at[k, pl.ds(low, rows), pl.ds(0, cols)], load_sem.at[k])
        for k, source in enumerate((f_in, g_in, s_in))
    ]
    loads.append(pltpu.make_async_copy(m_in, ext_m.at[pl.ds(low, rows), :], load_sem.at[3]))
    for copy in loads:
        copy.start()

    for copy in loads:
        copy.wait()

    packed = [[jnp.zeros((8, LANES), jnp.float32)] * per_chunk for _ in range(2)]
    for t in range(tiles):
        chunk, slot = divmod(t, per_chunk)
        here = pl.ds(low + 8 * t, 8)
        for f in range(FIELDS):
            group = chunk * FIELDS + f
            if f < 3:
                left, right = ext[f, here, :LANES], ext[f, here, cols - LANES : cols]
            else:
                left = ext_m[here, :LANES].astype(jnp.float32)
                right = ext_m[here, cols - LANES :].astype(jnp.float32)
            keep = lane // EDGE == group
            packed[0][slot] = jnp.where(keep, turn(left, EDGE * group), packed[0][slot])
            packed[1][slot] = jnp.where(keep, turn(right, EDGE * group + EDGE), packed[1][slot])
    for side in range(2):
        for slot in range(per_chunk):
            pack[side, 8 * slot : 8 * slot + 8, :] = packed[side][slot]

    @pl.when(fold)
    def _():
        last = pl.ds(high - 8, 8)
        count = cols // LANES
        for j in range(count):
            src = pl.ds((count - 1 - j) * LANES, LANES)
            dst = pl.ds(j * LANES, LANES)
            for f in range(3):
                flip_f[f, :, dst] = flip_tile(ext[f, last, src])
            flip_m[:, dst] = flip_tile(ext_m[last, src])
        for side in range(2):
            flip_c[side] = flip_tile(pack[side, top, :])

    @pl.when(bottom)
    def _():
        ext[:, 0:EDGE, 0:cols] = jnp.zeros((3, EDGE, cols), jnp.float32)
        ext_m[0:EDGE, :] = jnp.zeros((EDGE, cols), jnp.int32)
        corner[SW] = jnp.zeros((8, LANES), jnp.float32)
        corner[SE] = jnp.zeros((8, LANES), jnp.float32)

    pl.semaphore_wait(barrier, n - 1)

    south_rows, north_rows = pl.ds(0, EDGE), pl.ds(high, EDGE)
    body = pl.ds(0, cols)

    def send(src, dst, slot, order, target):
        return pltpu.make_async_remote_copy(
            src_ref=src, dst_ref=dst, send_sem=send_sem.at[order], recv_sem=recv_sem.at[slot],
            device_id=target, device_id_type=MESH_ID,
        )

    to_west = send(pack.at[0], came.at[0], 8, 0, (west, by))
    to_east = send(pack.at[1], came.at[1], 9, 1, (east, by))

    south = lax.max(by - 1, 0)
    first_rows = pl.ds(low, EDGE)
    last_rows = pl.ds(high - EDGE, EDGE)
    to_south = [
        send(pack.at[0, pl.ds(0, 8), :], corner.at[NE], NE, 4, (west, south)),
        send(pack.at[1, pl.ds(0, 8), :], corner.at[NW], NW, 5, (east, south)),
        send(ext.at[:, first_rows, body], ext.at[:, north_rows, body], 6, 2, (bx, south)),
        send(ext_m.at[first_rows, :], ext_m.at[north_rows, :], 7, 3, (bx, south)),
    ]
    north = lax.min(by + 1, nby - 1)
    to_north = [
        send(pack.at[0, top, :], corner.at[SE], SE, 8, (west, north)),
        send(pack.at[1, top, :], corner.at[SW], SW, 9, (east, north)),
        send(ext.at[:, last_rows, body], ext.at[:, south_rows, body], 4, 6, (bx, north)),
        send(ext_m.at[last_rows, :], ext_m.at[south_rows, :], 5, 7, (bx, north)),
    ]
    partner = nbx - 1 - bx
    partner_east = lax.rem(partner + 1, nbx)
    partner_west = lax.rem(partner + nbx - 1, nbx)
    over_fold = [
        send(flip_f, ext.at[:, north_rows, body], 6, 6, (partner, by)),
        send(flip_m, ext_m.at[north_rows, :], 7, 7, (partner, by)),
    ]
    fold_corners = [
        (send(flip_c.at[0], corner.at[NW], NW, 8, (partner_east, by)),
         pltpu.make_async_copy(flip_c.at[0], corner.at[NW], recv_sem.at[NW]), partner_east),
        (send(flip_c.at[1], corner.at[NE], NE, 9, (partner_west, by)),
         pltpu.make_async_copy(flip_c.at[1], corner.at[NE], recv_sem.at[NE]), partner_west),
    ]

    @pl.when(jnp.logical_not(bottom))
    def _():
        for copy in to_south[:2]:
            copy.start()

    @pl.when(jnp.logical_not(fold))
    def _():
        for copy in to_north[:2]:
            copy.start()

    to_west.start()
    to_east.start()

    @pl.when(jnp.logical_not(bottom))
    def _():
        for copy in to_south[2:]:
            copy.start()

    @pl.when(jnp.logical_not(fold))
    def _():
        for copy in to_north[2:]:
            copy.start()

    @pl.when(fold)
    def _():
        for copy in over_fold:
            copy.start()
        for remote, local, target in fold_corners:
            pl.when(target != bx)(remote.start)
            pl.when(target == bx)(local.start)

    to_west.wait_recv()
    to_east.wait_recv()

    for t in range(tiles):
        chunk, slot = divmod(t, per_chunk)
        here = pl.ds(low + 8 * t, 8)
        from_east = came[0, 8 * slot : 8 * slot + 8, :]
        from_west = came[1, 8 * slot : 8 * slot + 8, :]
        for f in range(FIELDS):
            group = chunk * FIELDS + f
            value = jnp.where(
                lane < EDGE,
                turn(from_east, -EDGE * group),
                jnp.where(lane >= LANES - EDGE, turn(from_west, -EDGE - EDGE * group), 0.0),
            )
            if f < 3:
                ext[f, here, cols:] = value
            else:
                mask[here, cols:] = value

    @pl.when(jnp.logical_not(bottom))
    def _():
        to_north[0].wait_recv()
        to_north[1].wait_recv()
        to_north[2].wait_recv()
        to_north[3].wait_recv()

    for copy in to_south:
        copy.wait_recv()

    corners = [corner[k] for k in range(4)]
    for f in range(FIELDS):
        group = top_chunk * FIELDS + f
        flipped = LANES // EDGE - 1 - group
        south_tile = jnp.where(
            lane < EDGE,
            turn(corners[SE], -EDGE * group),
            jnp.where(lane >= LANES - EDGE, turn(corners[SW], -EDGE - EDGE * group), 0.0),
        )
        north_east = jnp.where(
            fold, turn(corners[NE], -EDGE * flipped), turn(corners[NE], -EDGE * f)
        )
        north_west = jnp.where(
            fold, turn(corners[NW], -EDGE - EDGE * flipped), turn(corners[NW], -EDGE - EDGE * f)
        )
        north_tile = jnp.where(
            lane < EDGE, north_east, jnp.where(lane >= LANES - EDGE, north_west, 0.0)
        )
        if f < 3:
            ext[f, south_rows, cols:] = south_tile
            ext[f, north_rows, cols:] = north_tile
        else:
            mask[south_rows, cols:] = south_tile
            mask[north_rows, cols:] = north_tile
    mask[:, :cols] = ext_m[...].astype(jnp.float32)

    width = cols + LANES
    theta = (HIGH_BOUND + LOW_BOUND) / 2.0
    delta = (HIGH_BOUND - LOW_BOUND) / 2.0
    sigma = theta / delta
    rho = 1.0 / sigma

    wet = mask[...]
    diagonal = wet * (6.0 + ext[2])

    def apply(values):
        across = pltpu.roll(values, 1, 1) + pltpu.roll(values, width - 1, 1)
        column = values + 0.5 * across
        around = across + pltpu.roll(column, 1, 0) + pltpu.roll(column, whole - 1, 0)
        return diagonal * values - wet * around

    iterate = wet * ext[1]
    resid = wet * ext[0] - apply(iterate)
    direction = resid * (1.0 / theta)
    for sweep in range(ITERS):
        iterate = iterate + direction
        resid = resid - apply(direction)
        rho_next = 1.0 / (2.0 * sigma - rho)
        if sweep < ITERS - 1:
            direction = (rho_next * rho) * direction + (2.0 * rho_next / delta) * resid
        rho = rho_next

    final = resid[low:high, :cols]
    x_buf[...] = iterate[low:high, :cols]
    r_buf[...] = final

    square = final * final
    row_sums = jnp.sum(square, axis=1, keepdims=True)
    zero = jnp.zeros((8, 1), jnp.float32)
    pair = pair_tree([(row_sums[8 * t : 8 * t + 8], zero) for t in range(tiles)])
    pair = [jnp.broadcast_to(word, (8, LANES)) for word in pair]
    for step in (4, 2, 1):
        pair = pair_add(pair, [pltpu.roll(word, step, 0) for word in pair])
    part[...] = jnp.where(lane < LANES // 2, pair[0], pair[1])[0:1]

    for other in others:
        pltpu.make_async_remote_copy(
            src_ref=part, dst_ref=parts.at[me], send_sem=part_send.at[0], recv_sem=part_recv.at[0],
            device_id=other, device_id_type=MESH_ID,
        ).start()
    parts[me] = part[...]

    to_west.wait_send()
    to_east.wait_send()

    @pl.when(jnp.logical_not(bottom))
    def _():
        for copy in to_south:
            copy.wait_send()

    @pl.when(jnp.logical_not(fold))
    def _():
        for copy in to_north:
            copy.wait_send()

    @pl.when(fold)
    def _():
        for remote, local, target in fold_corners:
            pl.when(target != bx)(remote.wait_send)
        for copy in over_fold:
            copy.wait_send()

    bulk = parts.at[pl.ds(0, n - 1)]
    pltpu.make_async_copy(bulk, bulk, part_send.at[0]).wait()
    pltpu.make_async_copy(bulk, bulk, part_recv.at[0]).wait()

    def words(i):
        row = parts[i]
        return row, pltpu.roll(row, LANES // 2, 1)

    upper, lower = pair_tree([words(i) for i in range(n)])
    norm = jnp.sqrt((upper + lower) / (rows * cols * n))
    norm_out[...] = jnp.broadcast_to(norm, norm_out.shape)


def write_out(x_in, r_in, norm_in, x_out, r_out, norm_out, word, sem):
    word[...] = norm_in[0:1, 0:1]
    copies = [
        pltpu.make_async_copy(x_in, x_out, sem.at[0]),
        pltpu.make_async_copy(r_in, r_out, sem.at[1]),
        pltpu.make_async_copy(word, norm_out, sem.at[2]),
    ]
    for copy in copies:
        copy.start()
    for copy in copies:
        copy.wait()


def per_device(sizes, forcing, guess, shift, ocean_mask):
    nbx, nby, rows, cols = sizes
    n = nbx * nby
    whole, width = rows + 2 * EDGE, cols + LANES
    chunks = LANES // (FIELDS * EDGE)
    pack_rows = 8 * -(-(rows // 8) // chunks)
    f32 = jnp.float32
    hbm = pl.BlockSpec(memory_space=pl.ANY)
    vmem = pl.BlockSpec(memory_space=pltpu.VMEM)
    x, r, norm = pl.pallas_call(
        functools.partial(kernel, sizes),
        out_shape=(
            pltpu.VMEM((rows, cols), f32),
            pltpu.VMEM((rows, cols), f32),
            pltpu.VMEM((8, LANES), f32),
        ),
        in_specs=[hbm] * 4,
        out_specs=(vmem, vmem, vmem),
        scratch_shapes=[
            pltpu.VMEM((3, whole, width), f32),
            pltpu.VMEM((whole, cols), jnp.int32),
            pltpu.VMEM((whole, width), f32),
            pltpu.VMEM((3, EDGE, cols), f32),
            pltpu.VMEM((EDGE, cols), jnp.int32),
            pltpu.VMEM((2, pack_rows, LANES), f32),
            pltpu.VMEM((2, pack_rows, LANES), f32),
            pltpu.VMEM((4, 8, LANES), f32),
            pltpu.VMEM((2, 8, LANES), f32),
            pltpu.VMEM((1, LANES), f32),
            pltpu.VMEM((n, 1, LANES), f32),
            pltpu.SemaphoreType.DMA((4,)),
            pltpu.SemaphoreType.DMA((10,)),
            pltpu.SemaphoreType.DMA((10,)),
            pltpu.SemaphoreType.DMA((1,)),
            pltpu.SemaphoreType.DMA((1,)),
        ],
        compiler_params=pltpu.CompilerParams(collective_id=0, has_side_effects=True),
        name="chebyshev",
    )(forcing, guess, shift, ocean_mask)
    x = pltpu.with_memory_space_constraint(x, pltpu.VMEM)
    r = pltpu.with_memory_space_constraint(r, pltpu.VMEM)
    norm = pltpu.with_memory_space_constraint(norm, pltpu.VMEM)
    field = jax.ShapeDtypeStruct((rows, cols), f32)
    x, r, norm = pl.pallas_call(
        write_out,
        out_shape=(field, field, jax.ShapeDtypeStruct((1, 1), f32)),
        in_specs=[hbm, hbm, vmem],
        out_specs=(hbm,) * 3,
        scratch_shapes=[pltpu.VMEM((1, 1), f32), pltpu.SemaphoreType.DMA((3,))],
        name="write_out",
    )(x, r, norm)
    return x, r, norm.reshape(())


def solution(mesh):
    spec = P("by", "bx")
    nbx, nby = mesh.shape["bx"], mesh.shape["by"]

    def run(forcing, guess, shift, ocean_mask):
        sizes = (nbx, nby, forcing.shape[0] // nby, forcing.shape[1] // nbx)
        return jax.shard_map(
            functools.partial(per_device, sizes),
            mesh=mesh,
            in_specs=(spec,) * 4,
            out_specs=(spec, spec, P()),
            check_vma=False,
        )(forcing, guess, shift, ocean_mask)

    return run
```
